32 devices in a mesh: row: 4 (over y, x), th: 4 (over z), ph: 2 (over core).
Axes of the slice: x: 2, y: 2, z: 4, core: 2. Of those that a mesh axis runs over, the one named last changes fastest.
Arguments:
- cells: float32 [8, 16, 64, 256], P(None, 'row', 'th', 'ph'), may hold values from -2 to 3, as said below
- faces: float32 [3, 16, 64, 256], P(None, 'row', 'th', 'ph'), may hold values from -3 to 3
Outputs:
- state: float32 [8, 16, 64, 256], P(None, 'row', 'th', 'ph')
- faces_new: float32 [3, 16, 64, 256], P(None, 'row', 'th', 'ph')
The draws below stay inside these ranges and needn't reach their ends.
Inputs may be any that keep to these rules, and one draw needn't show every extreme that they name: `cells`: fields 0 and 4 (density, pressure) lie between 0.2 and 3; fields 1 to 3 between -0.5 and 0.5; fields 5 to 7 between -2 and 2.
All inputs are finite; a program needn't handle non-finite values.
Results may differ from the reference program's by a relative error of at most 0.0003.
Values sent between devices are 32-bit elements; how exact they have to be, the bound alone decides.
A program may use at most 64 MiB of HBM per device.

```python
import math
import jax
import jax.numpy as jnp
from jax import lax

CR = 4
NR = 16
NT = 64
NP = 256
N_ROW = 4


def draw_cells(key, part):
    keys = jax.random.split(key, 4)
    shape = (NR, NT, NP)
    rough_one = jax.random.uniform(keys[0], shape, jnp.float32)
    rough_two = jax.random.uniform(keys[1], shape, jnp.float32)
    density = 0.3 * jnp.exp(rough_one * math.log(10.0))
    pressure = 0.2 * jnp.exp(rough_two * math.log(10.0))
    velocity = jax.random.uniform(keys[2], (3,) + shape, jnp.float32, -0.5, 0.5)
    magnetic = jnp.clip(0.6 * jax.random.normal(keys[3], (3,) + shape, jnp.float32), -2.0, 2.0)
    return jnp.concatenate([density[None], velocity, pressure[None], magnetic], axis=0).astype(jnp.float32)


def level_of(rng, extent, pieces, low, top_value):
    def one(dim, parts):
        heights = jax.random.uniform(jax.random.fold_in(jax.random.fold_in(rng, 6), dim), (parts,), jnp.float32, low / len(pieces), top_value / len(pieces))
        return jnp.repeat(jnp.exp(heights), extent[dim] // parts).reshape((-1,) + (1,) * (len(extent) - dim - 1))

    gain = one(*pieces[0])
    for cut in pieces[1:]:
        gain = gain * one(*cut)
    return gain


def noise(key, dims, width, bound, shards=(), kind=jnp.bfloat16):
    drawn = width * jax.random.normal(key, dims, jnp.float32)
    if shards:
        drawn = drawn * level_of(key, dims, shards, -0.22, 0.18)
    return jnp.clip(drawn, -bound, bound).astype(kind)


def setup_inputs(seed: int = 0) -> dict:
    key_list = jax.random.split(jax.random.key(seed), 3)
    cells = draw_cells(jax.random.fold_in(key_list[2], 71), 0)
    faces = noise(key_list[1], (3, NR, NT, NP), 0.6, 3.0, ((1, 4), (2, 4), (3, 2)), jnp.float32)
    return {"cells": cells, "faces": faces}


adiabatic = 5.0 / 3.0
step_size = 0.05

def pad_ghosts(cells):
    field_ids = jnp.arange(cells.shape[0])
    flipper = jnp.where((field_ids == 2) | (field_ids == 7), -1.0, 1.0).astype(jnp.float32).reshape(-1, 1, 1, 1)
    padded = jnp.concatenate([cells[:, :, :, -1:], cells, cells[:, :, :, :1]], axis=3)
    padded = jnp.concatenate([padded[:, :, :1] * flipper, padded, padded[:, :, -1:] * flipper], axis=2)
    padded = jnp.concatenate([padded[:, :1], padded, padded[:, -1:]], axis=1)
    return padded

def conserved_flux(padded):
    density = padded[0]
    velocity = padded[1:4]
    pressure = padded[4]
    magnetic = padded[5:8]
    kinetic = 0.5 * density * lax.optimization_barrier(jnp.sum(velocity * velocity, axis=0))
    magnetic_sq = lax.optimization_barrier(jnp.sum(magnetic * magnetic, axis=0))
    energy = pressure / (adiabatic - 1.0) + kinetic + 0.5 * magnetic_sq
    total_press = pressure + 0.5 * magnetic_sq
    alignment = lax.optimization_barrier(jnp.sum(velocity * magnetic, axis=0))
    fast_speed = jnp.sqrt((adiabatic * pressure + magnetic_sq) / density)
    conserved = jnp.stack([density, density * velocity[0], density * velocity[1], density * velocity[2], energy])
    fluxes = []
    speeds = []
    for direction in range(3):
        moving = velocity[direction]
        normal_field = magnetic[direction]
        entries = [density * moving]
        for component in range(3):
            moment = density * velocity[component] * moving - magnetic[component] * normal_field
            if component == direction:
                moment = moment + total_press
            entries.append(moment)
        entries.append((energy + total_press) * moving - normal_field * alignment)
        fluxes.append(jnp.stack(entries))
        speeds.append(jnp.abs(moving) + fast_speed)
    return (conserved, fluxes, speeds)

def hydro_change(padded):
    conserved, fluxes, speeds = conserved_flux(padded)
    change = jnp.zeros_like(conserved[:, 1:-1, 1:-1, 1:-1])
    for direction in range(3):
        keeper = [slice(None), slice(1, -1), slice(1, -1), slice(1, -1)]
        keeper[direction + 1] = slice(None)
        lower_cut = [slice(None)] * 4
        upper_cut = [slice(None)] * 4
        lower_cut[direction + 1] = slice(0, -1)
        upper_cut[direction + 1] = slice(1, None)
        state_cut = conserved[tuple(keeper)]
        flux_cut = fluxes[direction][tuple(keeper)]
        speed_cut = speeds[direction][tuple(keeper[1:])]
        wave_speed = jnp.maximum(speed_cut[tuple(lower_cut[1:])], speed_cut[tuple(upper_cut[1:])])
        face_flux = 0.5 * (flux_cut[tuple(lower_cut)] + flux_cut[tuple(upper_cut)]) - 0.5 * wave_speed * (state_cut[tuple(upper_cut)] - state_cut[tuple(lower_cut)])
        change = change + face_flux[tuple(upper_cut)] - face_flux[tuple(lower_cut)]
    return conserved[:, 1:-1, 1:-1, 1:-1] - step_size * change

def edge_fields(padded):
    velocity = padded[1:4]
    magnetic = padded[5:8]
    emf_first = -(velocity[1] * magnetic[2] - velocity[2] * magnetic[1])
    emf_second = -(velocity[2] * magnetic[0] - velocity[0] * magnetic[2])
    emf_third = -(velocity[0] * magnetic[1] - velocity[1] * magnetic[0])
    inner = emf_first[1:-1]
    edge_one = 0.25 * (inner[:, :-1, :-1] + inner[:, 1:, :-1] + inner[:, :-1, 1:] + inner[:, 1:, 1:])
    inner = emf_second[:, 1:-1, :]
    edge_two = 0.25 * (inner[:-1, :, :-1] + inner[1:, :, :-1] + inner[:-1, :, 1:] + inner[1:, :, 1:])
    inner = emf_third[:, :, 1:-1]
    edge_three = 0.25 * (inner[:-1, :-1] + inner[1:, :-1] + inner[:-1, 1:] + inner[1:, 1:])
    return (edge_one, edge_two, edge_three)

def face_advance(first, second, third, edge_one, edge_two, edge_three):
    new_first = first - step_size * (edge_three[:, 1:] - edge_three[:, :-1] - (edge_two[:, :, 1:] - edge_two[:, :, :-1]))
    new_second = second - step_size * (edge_one[:, :, 1:] - edge_one[:, :, :-1] - (edge_three[1:] - edge_three[:-1]))
    new_third = third - step_size * (edge_two[1:] - edge_two[:-1] - (edge_one[:, 1:] - edge_one[:, :-1]))
    return (new_first, new_second, new_third)

def reference(cells, faces):
    padded = pad_ghosts(cells)
    first_ext = jnp.concatenate([faces[0], faces[0][-1:]], axis=0)
    second_ext = jnp.concatenate([faces[1], faces[1][:, -1:]], axis=1)
    third_ext = jnp.concatenate([faces[2], faces[2][:, :, :1]], axis=2)

    def slab(index):
        start = (index * CR).astype(jnp.int32)
        block = lax.dynamic_slice_in_dim(padded, start, CR + 2, 1)
        conserved_new = hydro_change(block)
        edge_one, edge_two, edge_three = edge_fields(block)
        first = lax.dynamic_slice_in_dim(first_ext, start, CR + 1, 0)
        second = lax.dynamic_slice_in_dim(second_ext, start, CR, 0)
        third = lax.dynamic_slice_in_dim(third_ext, start, CR, 0)
        new_first, new_second, new_third = face_advance(first, second, third, edge_one, edge_two, edge_three)
        return (conserved_new, new_first[:CR], new_second[:, :NT], new_third[:, :, :NP])
    outputs = lax.map(slab, jnp.arange(N_ROW, dtype=jnp.int32))
    conserved_new = jnp.moveaxis(outputs[0], 0, 1).reshape(5, NR, NT, NP)
    new_first = outputs[1].reshape(NR, NT, NP)
    new_second = outputs[2].reshape(NR, NT, NP)
    new_third = outputs[3].reshape(NR, NT, NP)
    upper_first = jnp.concatenate([new_first[1:], new_first[-1:]], axis=0)
    upper_second = jnp.concatenate([new_second[:, 1:], jnp.zeros((NR, 1, NP), jnp.float32)], axis=1)
    upper_third = jnp.concatenate([new_third[:, :, 1:], new_third[:, :, :1]], axis=2)
    centred = 0.5 * jnp.stack([new_first + upper_first, new_second + upper_second, new_third + upper_third])
    state = jnp.concatenate([conserved_new, centred], axis=0)
    return (state, jnp.stack([new_first, new_second, new_third]))
```

```python
import functools

import jax
import jax.numpy as jnp
from jax import lax
from jax.experimental import pallas as pl
from jax.experimental.pallas import tpu as pltpu
from jax.sharding import PartitionSpec as P

adiabatic = 5.0 / 3.0
step_size = 0.05
MESH = pl.DeviceIdType.MESH


def derived(prim, direction):
    density, velocity, pressure, magnetic = prim[0], prim[1:4], prim[4], prim[5:8]
    kinetic = 0.5 * density * (
        velocity[0] * velocity[0] + velocity[1] * velocity[1] + velocity[2] * velocity[2]
    )
    magnetic_sq = (
        magnetic[0] * magnetic[0] + magnetic[1] * magnetic[1] + magnetic[2] * magnetic[2]
    )
    energy = pressure / (adiabatic - 1.0) + kinetic + 0.5 * magnetic_sq
    total_press = pressure + 0.5 * magnetic_sq
    alignment = (
        velocity[0] * magnetic[0] + velocity[1] * magnetic[1] + velocity[2] * magnetic[2]
    )
    fast_speed = jnp.sqrt((adiabatic * pressure + magnetic_sq) / density)
    conserved = [density] + [density * v for v in velocity] + [energy]
    moving, normal_field = velocity[direction], magnetic[direction]
    flux = [conserved[1 + direction]]
    for component in range(3):
        moment = conserved[1 + component] * moving - magnetic[component] * normal_field
        if component == direction:
            moment = moment + total_press
        flux.append(moment)
    flux.append((energy + total_press) * moving - normal_field * alignment)
    return conserved, flux, jnp.abs(moving) + fast_speed


def face_flux(low, high):
    wave = 0.5 * jnp.maximum(low[2], high[2])
    return [
        0.5 * (low[1][i] + high[1][i]) - wave * (high[0][i] - low[0][i]) for i in range(5)
    ]


def emf_first(p):
    return p[3] * p[6] - p[2] * p[7]


def emf_second(p):
    return p[1] * p[7] - p[3] * p[5]


def emf_third(p):
    return p[2] * p[5] - p[1] * p[6]


def kernel(
    sizes,
    cells_hbm,
    faces_hbm,
    state,
    faces_new,
    cells,
    faces,
    from_ph,
    face_ph,
    pack_own,
    pack_ph,
    pack_row,
    from_th,
    face_th,
    from_thph,
    from_row,
    face_row,
    from_rowth,
    local_sem,
    send_sem,
    recv_sem,
):
    n_row, n_th, n_ph = sizes
    R, T, L = cells.shape[1:]
    half = L // 2
    row, th, ph = lax.axis_index("row"), lax.axis_index("th"), lax.axis_index("ph")
    at_bottom, at_top = row == 0, row == n_row - 1
    at_north, at_south = th == 0, th == n_th - 1
    left = lax.rem(ph + n_ph - 1, n_ph)
    right = lax.rem(ph + 1, n_ph)
    below, above = {"row": row - 1}, {"row": row + 1}
    north, south = {"th": th - 1}, {"th": th + 1}
    ph_targets = [{"ph": left}] if n_ph == 2 else [{"ph": left}, {"ph": right}]
    slots = len(ph_targets)

    barrier = pltpu.get_barrier_semaphore()
    greet = [
        (jnp.logical_not(at_bottom), below),
        (jnp.logical_not(at_top), above),
        (jnp.logical_not(at_north), north),
        (jnp.logical_not(at_south), south),
    ]
    for exists, who in greet:
        @pl.when(exists)
        def _():
            pl.semaphore_signal(barrier, inc=1, device_id=who, device_id_type=MESH)
    for who in ph_targets:
        pl.semaphore_signal(barrier, inc=1, device_id=who, device_id_type=MESH)

    load_cells = pltpu.make_async_copy(cells_hbm, cells, local_sem.at[0])
    load_faces = pltpu.make_async_copy(faces_hbm, faces, local_sem.at[1])
    load_cells.start()
    load_faces.start()

    count = [0]
    transfers = []

    def transfer(src, dst, who, sends=None, receives=None):
        index = count[0]
        count[0] += 1
        copy = pltpu.make_async_remote_copy(
            src_ref=src,
            dst_ref=dst,
            send_sem=send_sem.at[index],
            recv_sem=recv_sem.at[index],
            device_id=who,
            device_id_type=MESH,
        )

        def guarded(condition, action):
            if condition is None:
                action()
            else:
                pl.when(condition)(lambda: action())

        entry = (
            lambda: guarded(sends, copy.start),
            lambda: guarded(receives, copy.wait_recv),
            lambda: guarded(sends, copy.wait_send),
        )
        transfers.append(entry)
        return entry

    not_bottom, not_top, not_north, not_south = [g[0] for g in greet]
    first_row, last_row = pl.ds(0, 1), pl.ds(T - 1, 1)
    row_up = transfer(cells.at[:, R - 1], from_row.at[0], above, not_top, not_bottom)
    row_down = transfer(cells.at[:, 0], from_row.at[1], below, not_bottom, not_top)
    row_face = transfer(faces.at[0, 0], face_row, below, not_bottom, not_top)
    th_up = transfer(cells.at[:, :, last_row], from_th.at[0], south, not_south, not_north)
    th_down = transfer(cells.at[:, :, first_row], from_th.at[1], north, not_north, not_south)
    th_face = transfer(faces.at[1, :, first_row], face_th, north, not_north, not_south)
    ph_cells = [transfer(cells, from_ph.at[s], ph_targets[s]) for s in range(slots)]
    ph_pack = [transfer(pack_own, pack_ph.at[s], ph_targets[s]) for s in range(slots)]
    ph_face = transfer(faces.at[2], face_ph, ph_targets[0])
    corner = []
    for s in range(slots):
        corner.append(
            transfer(
                from_ph.at[s, pl.ds(2, 6), :, last_row], from_thph.at[s, 0], south, not_south, not_north
            )
        )
        corner.append(
            transfer(
                from_ph.at[s, pl.ds(2, 6), :, first_row], from_thph.at[s, 1], north, not_north, not_south
            )
        )
    packs = []
    for s in range(slots):
        packs.append(
            transfer(pack_ph.at[s, 1], pack_row.at[s, 0], above, not_top, not_bottom)
        )
        packs.append(
            transfer(pack_ph.at[s, 0], pack_row.at[s, 1], below, not_bottom, not_top)
        )
    rowth = []
    for side, has in ((0, not_north), (1, not_south)):
        rowth.append(
            transfer(
                from_th.at[side, pl.ds(1, 6), R - 1],
                from_rowth.at[0, side],
                above,
                jnp.logical_and(not_top, has),
                jnp.logical_and(not_bottom, has),
            )
        )
        rowth.append(
            transfer(
                from_th.at[side, pl.ds(1, 6), 0],
                from_rowth.at[1, side],
                below,
                jnp.logical_and(not_bottom, has),
                jnp.logical_and(not_top, has),
            )
        )

    lane = lax.broadcasted_iota(jnp.int32, (T, L), 1)
    sub = lax.broadcasted_iota(jnp.int32, (T, L), 0)

    load_cells.wait()
    for where, layer in ((0, 0), (1, R - 1)):
        e = emf_second([cells[f, layer] for f in range(8)])
        first_column = jnp.broadcast_to(e[:, :1], (T, L))
        last_column = jnp.broadcast_to(e[:, L - 1 :], (T, L))
        spread = jnp.where(lane == sub, first_column, 0.0) + jnp.where(
            lane == sub + half, last_column, 0.0
        )
        pack_own[where] = jnp.sum(spread, axis=0, keepdims=True)
    load_faces.wait()

    peers = slots + sum(exists.astype(jnp.int32) for exists, _ in greet)
    pl.semaphore_wait(barrier, peers)

    odd = lax.rem(row, 2) == 1

    @pl.when(odd)
    def _():
        row_up[0]()
        row_down[0]()

    @pl.when(jnp.logical_not(odd))
    def _():
        row_down[0]()
        row_up[0]()

    for t in [th_up, th_down] + ph_cells + ph_pack + [th_face, ph_face, row_face]:
        t[0]()
    for t in ph_cells + ph_pack:
        t[1]()
    for t in corner + packs:
        t[0]()
    for t in (th_up, th_down):
        t[1]()
    for t in rowth:
        t[0]()

    def flip(f, value):
        return -value if f in (2, 7) else value

    def own(r):
        return [cells[f, r] for f in range(8)]

    def beside(r):
        if slots == 1:
            return [from_ph[0, f, r] for f in range(8)]
        return [jnp.where(lane < half, from_ph[0, f, r], from_ph[1, f, r]) for f in range(8)]

    def th_low(r):
        x = [cells[f, r, :1] for f in range(8)]
        return [jnp.where(at_north, flip(f, x[f]), from_th[0, f, r]) for f in range(8)]

    def th_high(r):
        x = [cells[f, r, T - 1 :] for f in range(8)]
        return [jnp.where(at_south, flip(f, x[f]), from_th[1, f, r]) for f in range(8)]

    def th_prev(x, ghost):
        return jnp.where(sub == 0, jnp.broadcast_to(ghost, (T, L)), pltpu.roll(x, 1, 0))

    def th_next(x, ghost):
        return jnp.where(sub == T - 1, jnp.broadcast_to(ghost, (T, L)), pltpu.roll(x, T - 1, 0))

    def ph_prev(x, ghost):
        return pltpu.roll(jnp.where(lane == L - 1, ghost, x), 1, 1)

    def ph_next(x, ghost):
        return pltpu.roll(jnp.where(lane == 0, ghost, x), L - 1, 1)

    radial = []
    for r in range(R):
        x = own(r)
        g = beside(r)
        low, high = th_low(r), th_high(r)
        here = derived(x, 2)
        change = face_flux(here, derived([ph_next(a, b) for a, b in zip(x, g)], 2))
        other = face_flux(derived([ph_prev(a, b) for a, b in zip(x, g)], 2), here)
        change = [a - b for a, b in zip(change, other)]
        here = derived(x, 1)
        other = face_flux(here, derived([th_next(a, b) for a, b in zip(x, high)], 1))
        change = [a + b for a, b in zip(change, other)]
        other = face_flux(derived([th_prev(a, b) for a, b in zip(x, low)], 1), here)
        change = [a - b for a, b in zip(change, other)]
        here = derived(x, 0)
        if r:
            other = face_flux(derived(own(r - 1), 0), here)
            change = [a - b for a, b in zip(change, other)]
        if r < R - 1:
            other = face_flux(here, derived(own(r + 1), 0))
            change = [a + b for a, b in zip(change, other)]
        for i in range(5):
            state[i, r] = here[0][i] - step_size * change[i]

    for t in corner + [th_face, ph_face]:
        t[1]()

    def edge_first(r):
        x, g = own(r), beside(r)
        low, high = th_low(r), th_high(r)

        def beside_th(side, edge, at_pole):
            fields = [None, None]
            for f in range(2, 8):
                if slots == 1:
                    far = from_thph[0, side, f - 2, r]
                else:
                    far = jnp.where(
                        lane[:1] < half, from_thph[0, side, f - 2, r], from_thph[1, side, f - 2, r]
                    )
                fields.append(jnp.where(at_pole, flip(f, g[f][edge : edge + 1]), far))
            return fields

        e, eg = emf_first(x), emf_first(g)
        lower = e + th_prev(e, emf_first(low))
        upper = e + th_next(e, emf_first(high))
        lower_g = eg + th_prev(eg, emf_first(beside_th(0, 0, at_north)))
        upper_g = eg + th_next(eg, emf_first(beside_th(1, T - 1, at_south)))
        return (
            0.25 * (lower + ph_prev(lower, lower_g)),
            0.25 * (lower + ph_next(lower, lower_g)),
            0.25 * (upper + ph_prev(upper, upper_g)),
            0.25 * (upper + ph_next(upper, upper_g)),
        )

    def second_parts(r):
        return emf_second(own(r)), emf_second(beside(r))

    def third_parts(r):
        return emf_third(own(r)), emf_third(th_low(r)), emf_third(th_high(r))

    def edge_second(a, b):
        m, mg = a[0] + b[0], a[1] + b[1]
        return 0.25 * (m + ph_prev(m, mg)), 0.25 * (m + ph_next(m, mg))

    def edge_third(a, b):
        h, h_low, h_high = a[0] + b[0], a[1] + b[1], a[2] + b[2]
        return 0.25 * (h + th_prev(h, h_low)), 0.25 * (h + th_next(h, h_high))

    def advance_first(face, two, three):
        return face - step_size * (three[1] - three[0] - (two[1] - two[0]))

    twos, threes, firsts = {}, {}, {}
    for r in range(1, R):
        twos[r] = edge_second(second_parts(r - 1), second_parts(r))
        threes[r] = edge_third(third_parts(r - 1), third_parts(r))
        firsts[r] = advance_first(faces[0, r], twos[r], threes[r])

    def finish(r, ones):
        face = faces[1, r]
        second = face - step_size * (ones[1] - ones[0] - (threes[r + 1][0] - threes[r][0]))
        second_up = th_next(face, face_th[r]) - step_size * (
            ones[3] - ones[2] - (threes[r + 1][1] - threes[r][1])
        )
        second_up = jnp.where(jnp.logical_and(at_south, sub == T - 1), 0.0, second_up)
        face = faces[2, r]
        third = face - step_size * (twos[r + 1][0] - twos[r][0] - (ones[2] - ones[0]))
        third_up = ph_next(face, face_ph[r]) - step_size * (
            twos[r + 1][1] - twos[r][1] - (ones[3] - ones[1])
        )
        faces_new[1, r] = second
        faces_new[2, r] = third
        state[6, r] = 0.5 * (second + second_up)
        state[7, r] = 0.5 * (third + third_up)
        upper = firsts[r + 1]
        if r == R - 1:
            upper = jnp.where(at_top, firsts[r], upper)
        faces_new[0, r] = firsts[r]
        state[5, r] = 0.5 * (firsts[r] + upper)

    for r in range(1, R - 1):
        finish(r, edge_first(r))
    ones_low = edge_first(0)
    ones_high = edge_first(R - 1) if R > 1 else ones_low

    for t in packs + rowth + [row_up, row_down, row_face]:
        t[1]()

    def outer(side, at_end, r):
        x = own(r)
        ghost = [jnp.where(at_end, x[f], from_row[side, f]) for f in range(8)]

        def column(offset, s):
            spread = jnp.broadcast_to(pack_row[s, side], (T, L))
            return jnp.sum(jnp.where(lane == sub + offset, spread, 0.0), axis=1, keepdims=True)

        right_column, left_column = column(0, 0), column(half, slots - 1)
        far = jnp.where(
            lane < half,
            jnp.broadcast_to(right_column, (T, L)),
            jnp.broadcast_to(left_column, (T, L)),
        )
        far = jnp.where(at_end, emf_second(beside(r)), far)

        def th_ghost(which, edge, at_pole, own_ghost):
            fields = [None]
            for f in range(1, 7):
                value = jnp.where(at_end, own_ghost[f], from_rowth[side, which, f - 1])
                fields.append(jnp.where(at_pole, flip(f, ghost[f][edge : edge + 1]), value))
            return emf_third(fields)

        low = th_ghost(0, 0, at_north, th_low(r))
        high = th_ghost(1, T - 1, at_south, th_high(r))
        return ghost, (emf_second(ghost), far), (emf_third(ghost), low, high)

    ghost, two, three = outer(0, at_bottom, 0)
    flux = face_flux(derived(ghost, 0), derived(own(0), 0))
    for i in range(5):
        state[i, 0] = state[i, 0] + step_size * flux[i]
    twos[0] = edge_second(two, second_parts(0))
    threes[0] = edge_third(three, third_parts(0))
    firsts[0] = advance_first(faces[0, 0], twos[0], threes[0])

    ghost, two, three = outer(1, at_top, R - 1)
    flux = face_flux(derived(own(R - 1), 0), derived(ghost, 0))
    for i in range(5):
        state[i, R - 1] = state[i, R - 1] - step_size * flux[i]
    twos[R] = edge_second(second_parts(R - 1), two)
    threes[R] = edge_third(third_parts(R - 1), three)
    firsts[R] = advance_first(face_row[...], twos[R], threes[R])

    finish(0, ones_low)
    if R > 1:
        finish(R - 1, ones_high)

    for t in transfers:
        t[2]()


def on_device(sizes, cells, faces):
    fields, R, T, L = cells.shape
    slots = 1 if sizes[2] == 2 else 2
    f32 = jnp.float32
    copies = 7 + 4 + slots * 6
    return pl.pallas_call(
        functools.partial(kernel, sizes),
        out_shape=(
            jax.ShapeDtypeStruct(cells.shape, f32),
            jax.ShapeDtypeStruct(faces.shape, f32),
        ),
        in_specs=[pl.BlockSpec(memory_space=pl.ANY)] * 2,
        out_specs=[pl.BlockSpec(memory_space=pltpu.VMEM)] * 2,
        scratch_shapes=[
            pltpu.VMEM((fields, R, T, L), f32),
            pltpu.VMEM((3, R, T, L), f32),
            pltpu.VMEM((slots, fields, R, T, L), f32),
            pltpu.VMEM((R, T, L), f32),
            pltpu.VMEM((2, 1, L), f32),
            pltpu.VMEM((slots, 2, 1, L), f32),
            pltpu.VMEM((slots, 2, 1, L), f32),
            pltpu.VMEM((2, fields, R, 1, L), f32),
            pltpu.VMEM((R, 1, L), f32),
            pltpu.VMEM((slots, 2, 6, R, 1, L), f32),
            pltpu.VMEM((2, fields, T, L), f32),
            pltpu.VMEM((T, L), f32),
            pltpu.VMEM((2, 2, 6, 1, L), f32),
            pltpu.SemaphoreType.DMA((2,)),
            pltpu.SemaphoreType.DMA((copies,)),
            pltpu.SemaphoreType.DMA((copies,)),
        ],
        compiler_params=pltpu.CompilerParams(collective_id=0, has_side_effects=True),
    )(cells, faces)


def solution(mesh):
    sizes = (mesh.shape["row"], mesh.shape["th"], mesh.shape["ph"])
    place = P(None, "row", "th", "ph")
    return jax.shard_map(
        functools.partial(on_device, sizes),
        mesh=mesh,
        in_specs=(place, place),
        out_specs=(place, place),
        check_vma=False,
    )
```

```python
import functools

import jax
import jax.numpy as jnp
from jax import lax
from jax.experimental import pallas as pl
from jax.experimental.pallas import tpu as pltpu
from jax.sharding import PartitionSpec as P

adiabatic = 5.0 / 3.0
step_size = 0.05
MESH = pl.DeviceIdType.MESH


def derived(prim, direction):
    density, velocity, pressure, magnetic = prim[0], prim[1:4], prim[4], prim[5:8]
    kinetic = 0.5 * density * (
        velocity[0] * velocity[0] + velocity[1] * velocity[1] + velocity[2] * velocity[2]
    )
    magnetic_sq = (
        magnetic[0] * magnetic[0] + magnetic[1] * magnetic[1] + magnetic[2] * magnetic[2]
    )
    energy = pressure / (adiabatic - 1.0) + kinetic + 0.5 * magnetic_sq
    total_press = pressure + 0.5 * magnetic_sq
    alignment = (
        velocity[0] * magnetic[0] + velocity[1] * magnetic[1] + velocity[2] * magnetic[2]
    )
    fast_speed = jnp.sqrt((adiabatic * pressure + magnetic_sq) / density)
    conserved = [density] + [density * v for v in velocity] + [energy]
    moving, normal_field = velocity[direction], magnetic[direction]
    flux = [conserved[1 + direction]]
    for component in range(3):
        moment = conserved[1 + component] * moving - magnetic[component] * normal_field
        if component == direction:
            moment = moment + total_press
        flux.append(moment)
    flux.append((energy + total_press) * moving - normal_field * alignment)
    return conserved, flux, jnp.abs(moving) + fast_speed


def face_flux(low, high):
    wave = 0.5 * jnp.maximum(low[2], high[2])
    return [
        0.5 * (low[1][i] + high[1][i]) - wave * (high[0][i] - low[0][i]) for i in range(5)
    ]


def emf_first(p):
    return p[3] * p[6] - p[2] * p[7]


def emf_second(p):
    return p[1] * p[7] - p[3] * p[5]


def emf_third(p):
    return p[2] * p[5] - p[1] * p[6]


def kernel(
    sizes,
    cells_hbm,
    faces_hbm,
    state,
    faces_new,
    cells,
    faces,
    from_ph,
    face_ph,
    pack_own,
    pack_ph,
    pack_row,
    from_th,
    face_th,
    from_thph,
    from_row,
    face_row,
    from_rowth,
    local_sem,
    send_sem,
    recv_sem,
):
    n_row, n_th, n_ph = sizes
    R, T, L = cells.shape[1:]
    half = L // 2
    row, th, ph = lax.axis_index("row"), lax.axis_index("th"), lax.axis_index("ph")
    at_bottom, at_top = row == 0, row == n_row - 1
    at_north, at_south = th == 0, th == n_th - 1
    left = lax.rem(ph + n_ph - 1, n_ph)
    right = lax.rem(ph + 1, n_ph)
    below, above = {"row": row - 1}, {"row": row + 1}
    north, south = {"th": th - 1}, {"th": th + 1}
    ph_targets = [{"ph": left}] if n_ph == 2 else [{"ph": left}, {"ph": right}]
    slots = len(ph_targets)

    barrier = pltpu.get_barrier_semaphore()
    greet = [
        (jnp.logical_not(at_bottom), below),
        (jnp.logical_not(at_top), above),
        (jnp.logical_not(at_north), north),
        (jnp.logical_not(at_south), south),
    ]
    for exists, who in greet:
        @pl.when(exists)
        def _():
            pl.semaphore_signal(barrier, inc=1, device_id=who, device_id_type=MESH)
    for who in ph_targets:
        pl.semaphore_signal(barrier, inc=1, device_id=who, device_id_type=MESH)

    load_cells = pltpu.make_async_copy(cells_hbm, cells, local_sem.at[0])
    load_faces = pltpu.make_async_copy(faces_hbm, faces, local_sem.at[1])
    load_cells.start()
    load_faces.start()

    count = [0]
    transfers = []

    def transfer(src, dst, who, sends=None, receives=None):
        index = count[0]
        count[0] += 1
        copy = pltpu.make_async_remote_copy(
            src_ref=src,
            dst_ref=dst,
            send_sem=send_sem.at[index],
            recv_sem=recv_sem.at[index],
            device_id=who,
            device_id_type=MESH,
        )

        def guarded(condition, action):
            if condition is None:
                action()
            else:
                pl.when(condition)(lambda: action())

        entry = (
            lambda: guarded(sends, copy.start),
            lambda: guarded(receives, copy.wait_recv),
            lambda: guarded(sends, copy.wait_send),
        )
        transfers.append(entry)
        return entry

    not_bottom, not_top, not_north, not_south = [g[0] for g in greet]
    first_row, last_row = pl.ds(0, 1), pl.ds(T - 1, 1)
    row_up = transfer(cells.at[:, R - 1], from_row.at[0], above, not_top, not_bottom)
    row_down = transfer(cells.at[:, 0], from_row.at[1], below, not_bottom, not_top)
    row_face = transfer(faces.at[0, 0], face_row, below, not_bottom, not_top)
    th_up = transfer(cells.at[:, :, last_row], from_th.at[0], south, not_south, not_north)
    th_down = transfer(cells.at[:, :, first_row], from_th.at[1], north, not_north, not_south)
    th_face = transfer(faces.at[1, :, first_row], face_th, north, not_north, not_south)
    ph_cells = [transfer(cells, from_ph.at[s], ph_targets[s]) for s in range(slots)]
    ph_pack = [transfer(pack_own, pack_ph.at[s], ph_targets[s]) for s in range(slots)]
    ph_face = transfer(faces.at[2], face_ph, ph_targets[0])
    corner = []
    for s in range(slots):
        corner.append(
            transfer(
                from_ph.at[s, pl.ds(2, 6), :, last_row], from_thph.at[s, 0], south, not_south, not_north
            )
        )
        corner.append(
            transfer(
                from_ph.at[s, pl.ds(2, 6), :, first_row], from_thph.at[s, 1], north, not_north, not_south
            )
        )
    packs = []
    for s in range(slots):
        packs.append(
            transfer(pack_ph.at[s, 1], pack_row.at[s, 0], above, not_top, not_bottom)
        )
        packs.append(
            transfer(pack_ph.at[s, 0], pack_row.at[s, 1], below, not_bottom, not_top)
        )
    rowth = []
    for side, has in ((0, not_north), (1, not_south)):
        rowth.append(
            transfer(
                from_th.at[side, pl.ds(1, 6), R - 1],
                from_rowth.at[0, side],
                above,
                jnp.logical_and(not_top, has),
                jnp.logical_and(not_bottom, has),
            )
        )
        rowth.append(
            transfer(
                from_th.at[side, pl.ds(1, 6), 0],
                from_rowth.at[1, side],
                below,
                jnp.logical_and(not_bottom, has),
                jnp.logical_and(not_top, has),
            )
        )

    lane = lax.broadcasted_iota(jnp.int32, (T, L), 1)
    sub = lax.broadcasted_iota(jnp.int32, (T, L), 0)

    load_cells.wait()
    for where, layer in ((0, 0), (1, R - 1)):
        e = emf_second([cells[f, layer] for f in range(8)])
        first_column = jnp.broadcast_to(e[:, :1], (T, L))
        last_column = jnp.broadcast_to(e[:, L - 1 :], (T, L))
        spread = jnp.where(lane == sub, first_column, 0.0) + jnp.where(
            lane == sub + half, last_column, 0.0
        )
        pack_own[where] = jnp.sum(spread, axis=0, keepdims=True)
    load_faces.wait()

    peers = slots + sum(exists.astype(jnp.int32) for exists, _ in greet)
    pl.semaphore_wait(barrier, peers)

    odd = lax.rem(row, 2) == 1

    @pl.when(odd)
    def _():
        row_up[0]()
        row_down[0]()

    @pl.when(jnp.logical_not(odd))
    def _():
        row_down[0]()
        row_up[0]()

    for t in [th_up, th_down] + ph_cells + ph_pack + [th_face, ph_face, row_face]:
        t[0]()
    for t in ph_cells + ph_pack:
        t[1]()
    for t in corner + packs:
        t[0]()
    for t in (th_up, th_down):
        t[1]()
    for t in rowth:
        t[0]()

    def flip(f, value):
        return -value if f in (2, 7) else value

    def own(r):
        return [cells[f, r] for f in range(8)]

    def beside(r):
        if slots == 1:
            return [from_ph[0, f, r] for f in range(8)]
        return [jnp.where(lane < half, from_ph[0, f, r], from_ph[1, f, r]) for f in range(8)]

    def th_low(r):
        x = [cells[f, r, :1] for f in range(8)]
        return [jnp.where(at_north, flip(f, x[f]), from_th[0, f, r]) for f in range(8)]

    def th_high(r):
        x = [cells[f, r, T - 1 :] for f in range(8)]
        return [jnp.where(at_south, flip(f, x[f]), from_th[1, f, r]) for f in range(8)]

    def th_prev(x, ghost):
        return jnp.where(sub == 0, jnp.broadcast_to(ghost, (T, L)), pltpu.roll(x, 1, 0))

    def th_next(x, ghost):
        return jnp.where(sub == T - 1, jnp.broadcast_to(ghost, (T, L)), pltpu.roll(x, T - 1, 0))

    def ph_prev(x, ghost):
        return pltpu.roll(jnp.where(lane == L - 1, ghost, x), 1, 1)

    def ph_next(x, ghost):
        return pltpu.roll(jnp.where(lane == 0, ghost, x), L - 1, 1)

    radial = []
    for r in range(R):
        x = own(r)
        g = beside(r)
        low, high = th_low(r), th_high(r)
        here = derived(x, 2)
        change = face_flux(here, derived([ph_next(a, b) for a, b in zip(x, g)], 2))
        other = face_flux(derived([ph_prev(a, b) for a, b in zip(x, g)], 2), here)
        change = [a - b for a, b in zip(change, other)]
        here = derived(x, 1)
        other = face_flux(here, derived([th_next(a, b) for a, b in zip(x, high)], 1))
        change = [a + b for a, b in zip(change, other)]
        other = face_flux(derived([th_prev(a, b) for a, b in zip(x, low)], 1), here)
        change = [a - b for a, b in zip(change, other)]
        here = derived(x, 0)
        if r:
            other = face_flux(derived(own(r - 1), 0), here)
            change = [a - b for a, b in zip(change, other)]
        if r < R - 1:
            other = face_flux(here, derived(own(r + 1), 0))
            change = [a + b for a, b in zip(change, other)]
        for i in range(5):
            state[i, r] = here[0][i] - step_size * change[i]

    for t in corner + [th_face, ph_face]:
        t[1]()

    def edge_first(r):
        x, g = own(r), beside(r)
        low, high = th_low(r), th_high(r)

        def beside_th(side, edge, at_pole):
            fields = [None, None]
            for f in range(2, 8):
                if slots == 1:
                    far = from_thph[0, side, f - 2, r]
                else:
                    far = jnp.where(
                        lane[:1] < half, from_thph[0, side, f - 2, r], from_thph[1, side, f - 2, r]
                    )
                fields.append(jnp.where(at_pole, flip(f, g[f][edge : edge + 1]), far))
            return fields

        e, eg = emf_first(x), emf_first(g)
        lower = e + th_prev(e, emf_first(low))
        upper = e + th_next(e, emf_first(high))
        lower_g = eg + th_prev(eg, emf_first(beside_th(0, 0, at_north)))
        upper_g = eg + th_next(eg, emf_first(beside_th(1, T - 1, at_south)))
        return (
            0.25 * (lower + ph_prev(lower, lower_g)),
            0.25 * (lower + ph_next(lower, lower_g)),
            0.25 * (upper + ph_prev(upper, upper_g)),
            0.25 * (upper + ph_next(upper, upper_g)),
        )

    def second_parts(r):
        return emf_second(own(r)), emf_second(beside(r))

    def third_parts(r):
        return emf_third(own(r)), emf_third(th_low(r)), emf_third(th_high(r))

    def edge_second(a, b):
        m, mg = a[0] + b[0], a[1] + b[1]
        return 0.25 * (m + ph_prev(m, mg)), 0.25 * (m + ph_next(m, mg))

    def edge_third(a, b):
        h, h_low, h_high = a[0] + b[0], a[1] + b[1], a[2] + b[2]
        return 0.25 * (h + th_prev(h, h_low)), 0.25 * (h + th_next(h, h_high))

    def advance_first(face, two, three):
        return face - step_size * (three[1] - three[0] - (two[1] - two[0]))

    twos, threes, firsts = {}, {}, {}
    for r in range(1, R):
        twos[r] = edge_second(second_parts(r - 1), second_parts(r))
        threes[r] = edge_third(third_parts(r - 1), third_parts(r))
        firsts[r] = advance_first(faces[0, r], twos[r], threes[r])

    def finish(r, ones):
        face = faces[1, r]
        second = face - step_size * (ones[1] - ones[0] - (threes[r + 1][0] - threes[r][0]))
        second_up = th_next(face, face_th[r]) - step_size * (
            ones[3] - ones[2] - (threes[r + 1][1] - threes[r][1])
        )
        second_up = jnp.where(jnp.logical_and(at_south, sub == T - 1), 0.0, second_up)
        face = faces[2, r]
        third = face - step_size * (twos[r + 1][0] - twos[r][0] - (ones[2] - ones[0]))
        third_up = ph_next(face, face_ph[r]) - step_size * (
            twos[r + 1][1] - twos[r][1] - (ones[3] - ones[1])
        )
        faces_new[1, r] = second
        faces_new[2, r] = third
        state[6, r] = 0.5 * (second + second_up)
        state[7, r] = 0.5 * (third + third_up)
        upper = firsts[r + 1]
        if r == R - 1:
            upper = jnp.where(at_top, firsts[r], upper)
        faces_new[0, r] = firsts[r]
        state[5, r] = 0.5 * (firsts[r] + upper)

    for r in range(1, R - 1):
        finish(r, edge_first(r))
    ones_low = edge_first(0)
    ones_high = edge_first(R - 1) if R > 1 else ones_low

    for t in packs + rowth + [row_up, row_down, row_face]:
        t[1]()

    def outer(side, at_end, r):
        x = own(r)
        ghost = [jnp.where(at_end, x[f], from_row[side, f]) for f in range(8)]

        def column(offset, s):
            spread = jnp.broadcast_to(pack_row[s, side], (T, L))
            return jnp.sum(jnp.where(lane == sub + offset, spread, 0.0), axis=1, keepdims=True)

        right_column, left_column = column(0, 0), column(half, slots - 1)
        far = jnp.where(
            lane < half,
            jnp.broadcast_to(right_column, (T, L)),
            jnp.broadcast_to(left_column, (T, L)),
        )
        far = jnp.where(at_end, emf_second(beside(r)), far)

        def th_ghost(which, edge, at_pole, own_ghost):
            fields = [None]
            for f in range(1, 7):
                value = jnp.where(at_end, own_ghost[f], from_rowth[side, which, f - 1])
                fields.append(jnp.where(at_pole, flip(f, ghost[f][edge : edge + 1]), value))
            return emf_third(fields)

        low = th_ghost(0, 0, at_north, th_low(r))
        high = th_ghost(1, T - 1, at_south, th_high(r))
        return ghost, (emf_second(ghost), far), (emf_third(ghost), low, high)

    ghost, two, three = outer(0, at_bottom, 0)
    flux = face_flux(derived(ghost, 0), derived(own(0), 0))
    for i in range(5):
        state[i, 0] = state[i, 0] + step_size * flux[i]
    twos[0] = edge_second(two, second_parts(0))
    threes[0] = edge_third(three, third_parts(0))
    firsts[0] = advance_first(faces[0, 0], twos[0], threes[0])

    ghost, two, three = outer(1, at_top, R - 1)
    flux = face_flux(derived(own(R - 1), 0), derived(ghost, 0))
    for i in range(5):
        state[i, R - 1] = state[i, R - 1] - step_size * flux[i]
    twos[R] = edge_second(second_parts(R - 1), two)
    threes[R] = edge_third(third_parts(R - 1), three)
    firsts[R] = advance_first(face_row[...], twos[R], threes[R])

    finish(0, ones_low)
    if R > 1:
        finish(R - 1, ones_high)

    for t in transfers:
        t[2]()


def store(state, faces_new, state_hbm, faces_hbm, sem):
    copies = [
        pltpu.make_async_copy(state, state_hbm, sem.at[0]),
        pltpu.make_async_copy(faces_new, faces_hbm, sem.at[1]),
    ]
    for copy in copies:
        copy.start()
    for copy in copies:
        copy.wait()


def on_device(sizes, cells, faces):
    fields, R, T, L = cells.shape
    slots = 1 if sizes[2] == 2 else 2
    f32 = jnp.float32
    copies = 7 + 4 + slots * 6
    whole = (jax.ShapeDtypeStruct(cells.shape, f32), jax.ShapeDtypeStruct(faces.shape, f32))
    results = pl.pallas_call(
        functools.partial(kernel, sizes),
        out_shape=(pltpu.VMEM(cells.shape, f32), pltpu.VMEM(faces.shape, f32)),
        in_specs=[pl.BlockSpec(memory_space=pl.ANY)] * 2,
        out_specs=[pl.BlockSpec(memory_space=pltpu.VMEM)] * 2,
        scratch_shapes=[
            pltpu.VMEM((fields, R, T, L), f32),
            pltpu.VMEM((3, R, T, L), f32),
            pltpu.VMEM((slots, fields, R, T, L), f32),
            pltpu.VMEM((R, T, L), f32),
            pltpu.VMEM((2, 1, L), f32),
            pltpu.VMEM((slots, 2, 1, L), f32),
            pltpu.VMEM((slots, 2, 1, L), f32),
            pltpu.VMEM((2, fields, R, 1, L), f32),
            pltpu.VMEM((R, 1, L), f32),
            pltpu.VMEM((slots, 2, 6, R, 1, L), f32),
            pltpu.VMEM((2, fields, T, L), f32),
            pltpu.VMEM((T, L), f32),
            pltpu.VMEM((2, 2, 6, 1, L), f32),
            pltpu.SemaphoreType.DMA((2,)),
            pltpu.SemaphoreType.DMA((copies,)),
            pltpu.SemaphoreType.DMA((copies,)),
        ],
        compiler_params=pltpu.CompilerParams(collective_id=0, has_side_effects=True),
    )(cells, faces)
    return pl.pallas_call(
        store,
        out_shape=whole,
        in_specs=[pl.BlockSpec(memory_space=pltpu.VMEM)] * 2,
        out_specs=[pl.BlockSpec(memory_space=pl.ANY)] * 2,
        scratch_shapes=[pltpu.SemaphoreType.DMA((2,))],
    )(*[pltpu.with_memory_space_constraint(x, pltpu.VMEM) for x in results])


def solution(mesh):
    sizes = (mesh.shape["row"], mesh.shape["th"], mesh.shape["ph"])
    place = P(None, "row", "th", "ph")
    return jax.shard_map(
        functools.partial(on_device, sizes),
        mesh=mesh,
        in_specs=(place, place),
        out_specs=(place, place),
        check_vma=False,
    )
```

```python
import functools

import jax
import jax.numpy as jnp
from jax import lax
from jax.experimental import pallas as pl
from jax.experimental.pallas import tpu as pltpu
from jax.sharding import PartitionSpec as P

adiabatic = 5.0 / 3.0
step_size = 0.05
MESH = pl.DeviceIdType.MESH


def derived(prim, direction):
    density, velocity, pressure, magnetic = prim[0], prim[1:4], prim[4], prim[5:8]
    kinetic = 0.5 * density * (
        velocity[0] * velocity[0] + velocity[1] * velocity[1] + velocity[2] * velocity[2]
    )
    magnetic_sq = (
        magnetic[0] * magnetic[0] + magnetic[1] * magnetic[1] + magnetic[2] * magnetic[2]
    )
    energy = pressure / (adiabatic - 1.0) + kinetic + 0.5 * magnetic_sq
    total_press = pressure + 0.5 * magnetic_sq
    alignment = (
        velocity[0] * magnetic[0] + velocity[1] * magnetic[1] + velocity[2] * magnetic[2]
    )
    fast_speed = jnp.sqrt((adiabatic * pressure + magnetic_sq) / density)
    conserved = [density] + [density * v for v in velocity] + [energy]
    moving, normal_field = velocity[direction], magnetic[direction]
    flux = [conserved[1 + direction]]
    for component in range(3):
        moment = conserved[1 + component] * moving - magnetic[component] * normal_field
        if component == direction:
            moment = moment + total_press
        flux.append(moment)
    flux.append((energy + total_press) * moving - normal_field * alignment)
    return conserved, flux, jnp.abs(moving) + fast_speed


def face_flux(low, high):
    wave = 0.5 * jnp.maximum(low[2], high[2])
    return [
        0.5 * (low[1][i] + high[1][i]) - wave * (high[0][i] - low[0][i]) for i in range(5)
    ]


def emf_first(p):
    return p[3] * p[6] - p[2] * p[7]


def emf_second(p):
    return p[1] * p[7] - p[3] * p[5]


def emf_third(p):
    return p[2] * p[5] - p[1] * p[6]


def kernel(
    sizes,
    cells_hbm,
    faces_hbm,
    state,
    faces_new,
    cells,
    faces,
    from_ph,
    face_ph,
    pack_own,
    pack_row,
    from_th,
    face_th,
    from_thph,
    from_row,
    face_row,
    from_rowth,
    local_sem,
    send_sem,
    recv_sem,
):
    n_row, n_th, n_ph = sizes
    R, T, L = cells.shape[1:]
    half = L // 2
    row, th, ph = lax.axis_index("row"), lax.axis_index("th"), lax.axis_index("ph")
    at_bottom, at_top = row == 0, row == n_row - 1
    at_north, at_south = th == 0, th == n_th - 1
    left = lax.rem(ph + n_ph - 1, n_ph)
    right = lax.rem(ph + 1, n_ph)
    below, above = {"row": row - 1}, {"row": row + 1}
    north, south = {"th": th - 1}, {"th": th + 1}
    ph_targets = [{"ph": left}] if n_ph == 2 else [{"ph": left}, {"ph": right}]
    slots = len(ph_targets)

    odd = lax.rem(row, 2) == 1
    even = jnp.logical_not(odd)
    both = jnp.logical_and
    not_bottom, not_top = jnp.logical_not(at_bottom), jnp.logical_not(at_top)
    not_north, not_south = jnp.logical_not(at_north), jnp.logical_not(at_south)
    pair_up, pair_down = not_top, not_bottom

    barrier = pltpu.get_barrier_semaphore()
    sides = [(not_bottom, below), (not_top, above), (not_north, north), (not_south, south)]
    greet = list(sides)
    for who in ph_targets:
        greet.append((None, who))
        greet.extend((exists, {**side, **who}) for exists, side in sides)
    for pair, radial in ((pair_down, below), (pair_up, above)):
        for exists, polar in sides[2:]:
            greet.append((both(pair, exists), {**radial, **polar}))
    peers = slots
    for exists, who in greet:
        if exists is None:
            pl.semaphore_signal(barrier, inc=1, device_id=who, device_id_type=MESH)
        else:
            peers = peers + exists.astype(jnp.int32)

            @pl.when(exists)
            def _():
                pl.semaphore_signal(barrier, inc=1, device_id=who, device_id_type=MESH)

    load_cells = pltpu.make_async_copy(cells_hbm, cells, local_sem.at[0])
    load_faces = pltpu.make_async_copy(faces_hbm, faces, local_sem.at[1])
    load_cells.start()
    load_faces.start()

    count = [0]
    transfers = []

    def transfer(src, dst, who, sends=None, receives=None):
        index = count[0]
        count[0] += 1
        copy = pltpu.make_async_remote_copy(
            src_ref=src,
            dst_ref=dst,
            send_sem=send_sem.at[index],
            recv_sem=recv_sem.at[index],
            device_id=who,
            device_id_type=MESH,
        )

        def guarded(condition, action):
            if condition is None:
                action()
            else:
                pl.when(condition)(lambda: action())

        entry = (
            lambda: guarded(sends, copy.start),
            lambda: guarded(receives, copy.wait_recv),
            lambda: guarded(sends, copy.wait_send),
        )
        transfers.append(entry)
        return entry

    first_row, last_row = pl.ds(0, 1), pl.ds(T - 1, 1)
    row_up = transfer(cells.at[:, R - 1], from_row.at[0], above, not_top, not_bottom)
    row_down = transfer(cells.at[:, 0], from_row.at[1], below, not_bottom, not_top)
    row_face = transfer(faces.at[0, 0], face_row, below, not_bottom, not_top)
    th_up = transfer(cells.at[:, :, last_row], from_th.at[0], south, not_south, not_north)
    th_down = transfer(cells.at[:, :, first_row], from_th.at[1], north, not_north, not_south)
    th_face = transfer(faces.at[1, :, first_row], face_th, north, not_north, not_south)
    ph_cells = [transfer(cells, from_ph.at[s], ph_targets[s]) for s in range(slots)]
    ph_face = transfer(faces.at[2], face_ph, ph_targets[0])
    corner, packs = [], []
    for s in range(slots):
        who = ph_targets[s]
        for side, strip, towards, sends, receives in (
            (0, last_row, south, not_south, not_north),
            (1, first_row, north, not_north, not_south),
        ):
            src = cells.at[pl.ds(2, 6), :, strip]
            corner.append(
                transfer(src, from_thph.at[s, side], {**towards, **who}, sends, receives)
            )
        for side, towards, sends, receives in (
            (0, above, not_top, not_bottom),
            (1, below, not_bottom, not_top),
        ):
            src = pack_own.at[1 - side]
            packs.append(transfer(src, pack_row.at[s, side], {**towards, **who}, sends, receives))
    direct = []
    for side, layer, radial, sends_row, gets_row in (
        (0, R - 1, above, pair_up, pair_down),
        (1, 0, below, pair_down, pair_up),
    ):
        for where, strip, polar, sends_th, gets_th in (
            (0, last_row, south, not_south, not_north),
            (1, first_row, north, not_north, not_south),
        ):
            direct.append(
                transfer(
                    cells.at[pl.ds(1, 6), layer, strip],
                    from_rowth.at[side, where],
                    {**radial, **polar},
                    both(sends_row, sends_th),
                    both(gets_row, gets_th),
                )
            )

    lane = lax.broadcasted_iota(jnp.int32, (T, L), 1)
    sub = lax.broadcasted_iota(jnp.int32, (T, L), 0)

    load_cells.wait()
    for where, layer in ((0, 0), (1, R - 1)):
        e = emf_second([cells[f, layer] for f in range(8)])
        first_column = jnp.broadcast_to(e[:, :1], (T, L))
        last_column = jnp.broadcast_to(e[:, L - 1 :], (T, L))
        spread = jnp.where(lane == sub, first_column, 0.0) + jnp.where(
            lane == sub + half, last_column, 0.0
        )
        pack_own[where] = jnp.sum(spread, axis=0, keepdims=True)
    load_faces.wait()

    pl.semaphore_wait(barrier, peers)
    for t in ph_cells + direct + corner + [th_up, th_down] + packs:
        t[0]()

    @pl.when(odd)
    def _():
        for t in (row_down, row_face, row_up):
            t[0]()

    @pl.when(even)
    def _():
        for t in (row_up, row_down, row_face):
            t[0]()

    for t in (th_face, ph_face):
        t[0]()
    for t in ph_cells + [th_up, th_down]:
        t[1]()

    def flip(f, value):
        return -value if f in (2, 7) else value

    def own(r):
        return [cells[f, r] for f in range(8)]

    def beside(r):
        if slots == 1:
            return [from_ph[0, f, r] for f in range(8)]
        return [jnp.where(lane < half, from_ph[0, f, r], from_ph[1, f, r]) for f in range(8)]

    def th_low(r):
        x = [cells[f, r, :1] for f in range(8)]
        return [jnp.where(at_north, flip(f, x[f]), from_th[0, f, r]) for f in range(8)]

    def th_high(r):
        x = [cells[f, r, T - 1 :] for f in range(8)]
        return [jnp.where(at_south, flip(f, x[f]), from_th[1, f, r]) for f in range(8)]

    def th_prev(x, ghost):
        return jnp.where(sub == 0, jnp.broadcast_to(ghost, (T, L)), pltpu.roll(x, 1, 0))

    def th_next(x, ghost):
        return jnp.where(sub == T - 1, jnp.broadcast_to(ghost, (T, L)), pltpu.roll(x, T - 1, 0))

    def ph_prev(x, ghost):
        return pltpu.roll(jnp.where(lane == L - 1, ghost, x), 1, 1)

    def ph_next(x, ghost):
        return pltpu.roll(jnp.where(lane == 0, ghost, x), L - 1, 1)

    radial = []
    for r in range(R):
        x = own(r)
        g = beside(r)
        low, high = th_low(r), th_high(r)
        here = derived(x, 2)
        change = face_flux(here, derived([ph_next(a, b) for a, b in zip(x, g)], 2))
        other = face_flux(derived([ph_prev(a, b) for a, b in zip(x, g)], 2), here)
        change = [a - b for a, b in zip(change, other)]
        here = derived(x, 1)
        other = face_flux(here, derived([th_next(a, b) for a, b in zip(x, high)], 1))
        change = [a + b for a, b in zip(change, other)]
        other = face_flux(derived([th_prev(a, b) for a, b in zip(x, low)], 1), here)
        change = [a - b for a, b in zip(change, other)]
        here = derived(x, 0)
        if r:
            other = face_flux(derived(own(r - 1), 0), here)
            change = [a - b for a, b in zip(change, other)]
        if r < R - 1:
            other = face_flux(here, derived(own(r + 1), 0))
            change = [a + b for a, b in zip(change, other)]
        for i in range(5):
            state[i, r] = here[0][i] - step_size * change[i]

    for t in corner + [th_face, ph_face]:
        t[1]()

    def edge_first(r):
        x, g = own(r), beside(r)
        low, high = th_low(r), th_high(r)

        def beside_th(side, edge, at_pole):
            fields = [None, None]
            for f in range(2, 8):
                if slots == 1:
                    far = from_thph[0, side, f - 2, r]
                else:
                    far = jnp.where(
                        lane[:1] < half, from_thph[0, side, f - 2, r], from_thph[1, side, f - 2, r]
                    )
                fields.append(jnp.where(at_pole, flip(f, g[f][edge : edge + 1]), far))
            return fields

        e, eg = emf_first(x), emf_first(g)
        lower = e + th_prev(e, emf_first(low))
        upper = e + th_next(e, emf_first(high))
        lower_g = eg + th_prev(eg, emf_first(beside_th(0, 0, at_north)))
        upper_g = eg + th_next(eg, emf_first(beside_th(1, T - 1, at_south)))
        return (
            0.25 * (lower + ph_prev(lower, lower_g)),
            0.25 * (lower + ph_next(lower, lower_g)),
            0.25 * (upper + ph_prev(upper, upper_g)),
            0.25 * (upper + ph_next(upper, upper_g)),
        )

    def second_parts(r):
        return emf_second(own(r)), emf_second(beside(r))

    def third_parts(r):
        return emf_third(own(r)), emf_third(th_low(r)), emf_third(th_high(r))

    def edge_second(a, b):
        m, mg = a[0] + b[0], a[1] + b[1]
        return 0.25 * (m + ph_prev(m, mg)), 0.25 * (m + ph_next(m, mg))

    def edge_third(a, b):
        h, h_low, h_high = a[0] + b[0], a[1] + b[1], a[2] + b[2]
        return 0.25 * (h + th_prev(h, h_low)), 0.25 * (h + th_next(h, h_high))

    def advance_first(face, two, three):
        return face - step_size * (three[1] - three[0] - (two[1] - two[0]))

    twos, threes, firsts = {}, {}, {}
    for r in range(1, R):
        twos[r] = edge_second(second_parts(r - 1), second_parts(r))
        threes[r] = edge_third(third_parts(r - 1), third_parts(r))
        firsts[r] = advance_first(faces[0, r], twos[r], threes[r])

    def finish(r, ones):
        face = faces[1, r]
        second = face - step_size * (ones[1] - ones[0] - (threes[r + 1][0] - threes[r][0]))
        second_up = th_next(face, face_th[r]) - step_size * (
            ones[3] - ones[2] - (threes[r + 1][1] - threes[r][1])
        )
        second_up = jnp.where(jnp.logical_and(at_south, sub == T - 1), 0.0, second_up)
        face = faces[2, r]
        third = face - step_size * (twos[r + 1][0] - twos[r][0] - (ones[2] - ones[0]))
        third_up = ph_next(face, face_ph[r]) - step_size * (
            twos[r + 1][1] - twos[r][1] - (ones[3] - ones[1])
        )
        faces_new[1, r] = second
        faces_new[2, r] = third
        state[6, r] = 0.5 * (second + second_up)
        state[7, r] = 0.5 * (third + third_up)
        upper = firsts[r + 1]
        if r == R - 1:
            upper = jnp.where(at_top, firsts[r], upper)
        faces_new[0, r] = firsts[r]
        state[5, r] = 0.5 * (firsts[r] + upper)

    for r in range(1, R - 1):
        finish(r, edge_first(r))
    ones_low = edge_first(0)
    ones_high = edge_first(R - 1) if R > 1 else ones_low

    for t in packs + direct + [row_up, row_down, row_face]:
        t[1]()

    def outer(side, at_end, r):
        x = own(r)
        ghost = [jnp.where(at_end, x[f], from_row[side, f]) for f in range(8)]

        def column(offset, s):
            spread = jnp.broadcast_to(pack_row[s, side], (T, L))
            return jnp.sum(jnp.where(lane == sub + offset, spread, 0.0), axis=1, keepdims=True)

        right_column, left_column = column(0, 0), column(half, slots - 1)
        far = jnp.where(
            lane < half,
            jnp.broadcast_to(right_column, (T, L)),
            jnp.broadcast_to(left_column, (T, L)),
        )
        far = jnp.where(at_end, emf_second(beside(r)), far)

        def th_ghost(which, edge, at_pole, own_ghost):
            fields = [None]
            for f in range(1, 7):
                value = jnp.where(at_end, own_ghost[f], from_rowth[side, which, f - 1])
                fields.append(jnp.where(at_pole, flip(f, ghost[f][edge : edge + 1]), value))
            return emf_third(fields)

        low = th_ghost(0, 0, at_north, th_low(r))
        high = th_ghost(1, T - 1, at_south, th_high(r))
        return ghost, (emf_second(ghost), far), (emf_third(ghost), low, high)

    ghost, two, three = outer(0, at_bottom, 0)
    flux = face_flux(derived(ghost, 0), derived(own(0), 0))
    for i in range(5):
        state[i, 0] = state[i, 0] + step_size * flux[i]
    twos[0] = edge_second(two, second_parts(0))
    threes[0] = edge_third(three, third_parts(0))
    firsts[0] = advance_first(faces[0, 0], twos[0], threes[0])

    ghost, two, three = outer(1, at_top, R - 1)
    flux = face_flux(derived(own(R - 1), 0), derived(ghost, 0))
    for i in range(5):
        state[i, R - 1] = state[i, R - 1] - step_size * flux[i]
    twos[R] = edge_second(second_parts(R - 1), two)
    threes[R] = edge_third(third_parts(R - 1), three)
    firsts[R] = advance_first(face_row[...], twos[R], threes[R])

    finish(0, ones_low)
    if R > 1:
        finish(R - 1, ones_high)

    for t in transfers:
        t[2]()


def store(state, faces_new, state_hbm, faces_hbm, sem):
    copies = [
        pltpu.make_async_copy(state, state_hbm, sem.at[0]),
        pltpu.make_async_copy(faces_new, faces_hbm, sem.at[1]),
    ]
    for copy in copies:
        copy.start()
    for copy in copies:
        copy.wait()


def on_device(sizes, cells, faces):
    fields, R, T, L = cells.shape
    slots = 1 if sizes[2] == 2 else 2
    f32 = jnp.float32
    copies = 11 + slots * 5
    whole = (jax.ShapeDtypeStruct(cells.shape, f32), jax.ShapeDtypeStruct(faces.shape, f32))
    results = pl.pallas_call(
        functools.partial(kernel, sizes),
        out_shape=(pltpu.VMEM(cells.shape, f32), pltpu.VMEM(faces.shape, f32)),
        in_specs=[pl.BlockSpec(memory_space=pl.ANY)] * 2,
        out_specs=[pl.BlockSpec(memory_space=pltpu.VMEM)] * 2,
        scratch_shapes=[
            pltpu.VMEM((fields, R, T, L), f32),
            pltpu.VMEM((3, R, T, L), f32),
            pltpu.VMEM((slots, fields, R, T, L), f32),
            pltpu.VMEM((R, T, L), f32),
            pltpu.VMEM((2, 1, L), f32),
            pltpu.VMEM((slots, 2, 1, L), f32),
            pltpu.VMEM((2, fields, R, 1, L), f32),
            pltpu.VMEM((R, 1, L), f32),
            pltpu.VMEM((slots, 2, 6, R, 1, L), f32),
            pltpu.VMEM((2, fields, T, L), f32),
            pltpu.VMEM((T, L), f32),
            pltpu.VMEM((2, 2, 6, 1, L), f32),
            pltpu.SemaphoreType.DMA((2,)),
            pltpu.SemaphoreType.DMA((copies,)),
            pltpu.SemaphoreType.DMA((copies,)),
        ],
        compiler_params=pltpu.CompilerParams(collective_id=0, has_side_effects=True),
    )(cells, faces)
    return pl.pallas_call(
        store,
        out_shape=whole,
        in_specs=[pl.BlockSpec(memory_space=pltpu.VMEM)] * 2,
        out_specs=[pl.BlockSpec(memory_space=pl.ANY)] * 2,
        scratch_shapes=[pltpu.SemaphoreType.DMA((2,))],
    )(*[pltpu.with_memory_space_constraint(x, pltpu.VMEM) for x in results])


def solution(mesh):
    sizes = (mesh.shape["row"], mesh.shape["th"], mesh.shape["ph"])
    place = P(None, "row", "th", "ph")
    return jax.shard_map(
        functools.partial(on_device, sizes),
        mesh=mesh,
        in_specs=(place, place),
        out_specs=(place, place),
        check_vma=False,
    )
```

```python
import functools

import jax
import jax.numpy as jnp
from jax import lax
from jax.experimental import pallas as pl
from jax.experimental.pallas import tpu as pltpu
from jax.sharding import PartitionSpec as P

adiabatic = 5.0 / 3.0
step_size = 0.05
MESH = pl.DeviceIdType.MESH


def derived(prim, direction):
    density, velocity, pressure, magnetic = prim[0], prim[1:4], prim[4], prim[5:8]
    kinetic = 0.5 * density * (
        velocity[0] * velocity[0] + velocity[1] * velocity[1] + velocity[2] * velocity[2]
    )
    magnetic_sq = (
        magnetic[0] * magnetic[0] + magnetic[1] * magnetic[1] + magnetic[2] * magnetic[2]
    )
    energy = pressure / (adiabatic - 1.0) + kinetic + 0.5 * magnetic_sq
    total_press = pressure + 0.5 * magnetic_sq
    alignment = (
        velocity[0] * magnetic[0] + velocity[1] * magnetic[1] + velocity[2] * magnetic[2]
    )
    fast_speed = jnp.sqrt((adiabatic * pressure + magnetic_sq) / density)
    conserved = [density] + [density * v for v in velocity] + [energy]
    moving, normal_field = velocity[direction], magnetic[direction]
    flux = [conserved[1 + direction]]
    for component in range(3):
        moment = conserved[1 + component] * moving - magnetic[component] * normal_field
        if component == direction:
            moment = moment + total_press
        flux.append(moment)
    flux.append((energy + total_press) * moving - normal_field * alignment)
    return conserved, flux, jnp.abs(moving) + fast_speed


def face_flux(low, high):
    wave = 0.5 * jnp.maximum(low[2], high[2])
    return [
        0.5 * (low[1][i] + high[1][i]) - wave * (high[0][i] - low[0][i]) for i in range(5)
    ]


def emf_first(p):
    return p[3] * p[6] - p[2] * p[7]


def emf_second(p):
    return p[1] * p[7] - p[3] * p[5]


def emf_third(p):
    return p[2] * p[5] - p[1] * p[6]


def kernel(
    sizes,
    cells_hbm,
    faces_hbm,
    state,
    faces_new,
    cells,
    faces,
    from_ph,
    face_ph,
    pack_own,
    pack_row,
    from_th,
    face_th,
    from_thph,
    from_row,
    face_row,
    from_rowth,
    local_sem,
    send_sem,
    recv_sem,
):
    n_row, n_th, n_ph = sizes
    R, T, L = cells.shape[1:]
    half = L // 2
    row, th, ph = lax.axis_index("row"), lax.axis_index("th"), lax.axis_index("ph")
    at_bottom, at_top = row == 0, row == n_row - 1
    at_north, at_south = th == 0, th == n_th - 1
    left = lax.rem(ph + n_ph - 1, n_ph)
    right = lax.rem(ph + 1, n_ph)
    below, above = {"row": row - 1}, {"row": row + 1}
    north, south = {"th": th - 1}, {"th": th + 1}
    ph_targets = [{"ph": left}] if n_ph == 2 else [{"ph": left}, {"ph": right}]
    slots = len(ph_targets)

    odd = lax.rem(row, 2) == 1
    even = jnp.logical_not(odd)
    both = jnp.logical_and
    not_bottom, not_top = jnp.logical_not(at_bottom), jnp.logical_not(at_top)
    not_north, not_south = jnp.logical_not(at_north), jnp.logical_not(at_south)
    pair_up, pair_down = not_top, not_bottom

    barrier = pltpu.get_barrier_semaphore()
    sides = [(not_bottom, below), (not_top, above), (not_north, north), (not_south, south)]
    greet = list(sides)
    for who in ph_targets:
        greet.append((None, who))
        greet.extend((exists, {**side, **who}) for exists, side in sides)
    for pair, radial in ((pair_down, below), (pair_up, above)):
        for exists, polar in sides[2:]:
            greet.append((both(pair, exists), {**radial, **polar}))
    peers = slots
    for exists, who in greet:
        if exists is None:
            pl.semaphore_signal(barrier, inc=1, device_id=who, device_id_type=MESH)
        else:
            peers = peers + exists.astype(jnp.int32)

            @pl.when(exists)
            def _():
                pl.semaphore_signal(barrier, inc=1, device_id=who, device_id_type=MESH)

    load_cells = pltpu.make_async_copy(cells_hbm, cells, local_sem.at[0])
    load_faces = pltpu.make_async_copy(faces_hbm, faces, local_sem.at[1])
    load_cells.start()
    load_faces.start()

    count = [0]
    transfers = []

    def transfer(src, dst, who, sends=None, receives=None):
        index = count[0]
        count[0] += 1
        copy = pltpu.make_async_remote_copy(
            src_ref=src,
            dst_ref=dst,
            send_sem=send_sem.at[index],
            recv_sem=recv_sem.at[index],
            device_id=who,
            device_id_type=MESH,
        )

        def guarded(condition, action):
            if condition is None:
                action()
            else:
                pl.when(condition)(lambda: action())

        entry = (
            lambda: guarded(sends, copy.start),
            lambda: guarded(receives, copy.wait_recv),
            lambda: guarded(sends, copy.wait_send),
        )
        transfers.append(entry)
        return entry

    first_row, last_row = pl.ds(0, 1), pl.ds(T - 1, 1)
    row_up = transfer(cells.at[:, R - 1], from_row.at[0], above, not_top, not_bottom)
    row_down = transfer(cells.at[:, 0], from_row.at[1], below, not_bottom, not_top)
    row_face = transfer(faces.at[0, 0], face_row, below, not_bottom, not_top)
    th_up = transfer(cells.at[:, :, last_row], from_th.at[0], south, not_south, not_north)
    th_down = transfer(cells.at[:, :, first_row], from_th.at[1], north, not_north, not_south)
    th_face = transfer(faces.at[1, :, first_row], face_th, north, not_north, not_south)
    ph_cells = [transfer(cells, from_ph.at[s], ph_targets[s]) for s in range(slots)]
    ph_face = transfer(faces.at[2], face_ph, ph_targets[0])
    corner, packs = [], []
    for s in range(slots):
        who = ph_targets[s]
        for side, strip, towards, sends, receives in (
            (0, last_row, south, not_south, not_north),
            (1, first_row, north, not_north, not_south),
        ):
            src = cells.at[pl.ds(2, 6), :, strip]
            corner.append(
                transfer(src, from_thph.at[s, side], {**towards, **who}, sends, receives)
            )
        for side, towards, sends, receives in (
            (0, above, not_top, not_bottom),
            (1, below, not_bottom, not_top),
        ):
            src = pack_own.at[1 - side]
            packs.append(transfer(src, pack_row.at[s, side], {**towards, **who}, sends, receives))
    direct = []
    for side, layer, radial, sends_row, gets_row in (
        (0, R - 1, above, pair_up, pair_down),
        (1, 0, below, pair_down, pair_up),
    ):
        for where, strip, polar, sends_th, gets_th in (
            (0, last_row, south, not_south, not_north),
            (1, first_row, north, not_north, not_south),
        ):
            direct.append(
                transfer(
                    cells.at[pl.ds(1, 6), layer, strip],
                    from_rowth.at[side, where],
                    {**radial, **polar},
                    both(sends_row, sends_th),
                    both(gets_row, gets_th),
                )
            )

    lane = lax.broadcasted_iota(jnp.int32, (T, L), 1)
    sub = lax.broadcasted_iota(jnp.int32, (T, L), 0)

    load_cells.wait()
    for where, layer in ((0, 0), (1, R - 1)):
        e = emf_second([cells[f, layer] for f in range(8)])
        first_column = jnp.broadcast_to(e[:, :1], (T, L))
        last_column = jnp.broadcast_to(e[:, L - 1 :], (T, L))
        spread = jnp.where(lane == sub, first_column, 0.0) + jnp.where(
            lane == sub + half, last_column, 0.0
        )
        pack_own[where] = jnp.sum(spread, axis=0, keepdims=True)
    load_faces.wait()

    pl.semaphore_wait(barrier, peers)
    for t in ph_cells + direct + corner + [th_up, th_down] + packs:
        t[0]()

    @pl.when(odd)
    def _():
        for t in (row_down, row_face):
            t[0]()

    @pl.when(even)
    def _():
        row_up[0]()

    for t in (th_face, ph_face):
        t[0]()
    for t in ph_cells:
        t[1]()

    @pl.when(odd)
    def _():
        row_up[0]()

    @pl.when(even)
    def _():
        for t in (row_down, row_face):
            t[0]()

    def flip(f, value):
        return -value if f in (2, 7) else value

    def own(r):
        return [cells[f, r] for f in range(8)]

    def beside(r):
        if slots == 1:
            return [from_ph[0, f, r] for f in range(8)]
        return [jnp.where(lane < half, from_ph[0, f, r], from_ph[1, f, r]) for f in range(8)]

    def th_low(r):
        x = [cells[f, r, :1] for f in range(8)]
        return [jnp.where(at_north, flip(f, x[f]), from_th[0, f, r]) for f in range(8)]

    def th_high(r):
        x = [cells[f, r, T - 1 :] for f in range(8)]
        return [jnp.where(at_south, flip(f, x[f]), from_th[1, f, r]) for f in range(8)]

    def th_prev(x, ghost):
        return jnp.where(sub == 0, jnp.broadcast_to(ghost, (T, L)), pltpu.roll(x, 1, 0))

    def th_next(x, ghost):
        return jnp.where(sub == T - 1, jnp.broadcast_to(ghost, (T, L)), pltpu.roll(x, T - 1, 0))

    def ph_prev(x, ghost):
        return pltpu.roll(jnp.where(lane == L - 1, ghost, x), 1, 1)

    def ph_next(x, ghost):
        return pltpu.roll(jnp.where(lane == 0, ghost, x), L - 1, 1)

    for r in range(R):
        x, g = own(r), beside(r)
        here = derived(x, 2)
        change = face_flux(here, derived([ph_next(a, b) for a, b in zip(x, g)], 2))
        other = face_flux(derived([ph_prev(a, b) for a, b in zip(x, g)], 2), here)
        change = [a - b for a, b in zip(change, other)]
        here = derived(x, 0)
        if r:
            other = face_flux(derived(own(r - 1), 0), here)
            change = [a - b for a, b in zip(change, other)]
        if r < R - 1:
            other = face_flux(here, derived(own(r + 1), 0))
            change = [a + b for a, b in zip(change, other)]
        for i in range(5):
            state[i, r] = here[0][i] - step_size * change[i]

    for t in (th_up, th_down):
        t[1]()
    for r in range(R):
        x, low, high = own(r), th_low(r), th_high(r)
        here = derived(x, 1)
        change = face_flux(here, derived([th_next(a, b) for a, b in zip(x, high)], 1))
        other = face_flux(derived([th_prev(a, b) for a, b in zip(x, low)], 1), here)
        for i in range(5):
            state[i, r] = state[i, r] - step_size * (change[i] - other[i])

    for t in corner + [th_face, ph_face]:
        t[1]()

    def edge_first(r):
        x, g = own(r), beside(r)
        low, high = th_low(r), th_high(r)

        def beside_th(side, edge, at_pole):
            fields = [None, None]
            for f in range(2, 8):
                if slots == 1:
                    far = from_thph[0, side, f - 2, r]
                else:
                    far = jnp.where(
                        lane[:1] < half, from_thph[0, side, f - 2, r], from_thph[1, side, f - 2, r]
                    )
                fields.append(jnp.where(at_pole, flip(f, g[f][edge : edge + 1]), far))
            return fields

        e, eg = emf_first(x), emf_first(g)
        lower = e + th_prev(e, emf_first(low))
        upper = e + th_next(e, emf_first(high))
        lower_g = eg + th_prev(eg, emf_first(beside_th(0, 0, at_north)))
        upper_g = eg + th_next(eg, emf_first(beside_th(1, T - 1, at_south)))
        return (
            0.25 * (lower + ph_prev(lower, lower_g)),
            0.25 * (lower + ph_next(lower, lower_g)),
            0.25 * (upper + ph_prev(upper, upper_g)),
            0.25 * (upper + ph_next(upper, upper_g)),
        )

    def second_parts(r):
        return emf_second(own(r)), emf_second(beside(r))

    def third_parts(r):
        return emf_third(own(r)), emf_third(th_low(r)), emf_third(th_high(r))

    def edge_second(a, b):
        m, mg = a[0] + b[0], a[1] + b[1]
        return 0.25 * (m + ph_prev(m, mg)), 0.25 * (m + ph_next(m, mg))

    def edge_third(a, b):
        h, h_low, h_high = a[0] + b[0], a[1] + b[1], a[2] + b[2]
        return 0.25 * (h + th_prev(h, h_low)), 0.25 * (h + th_next(h, h_high))

    def advance_first(face, two, three):
        return face - step_size * (three[1] - three[0] - (two[1] - two[0]))

    twos, threes, firsts = {}, {}, {}
    for r in range(1, R):
        twos[r] = edge_second(second_parts(r - 1), second_parts(r))
        threes[r] = edge_third(third_parts(r - 1), third_parts(r))
        firsts[r] = advance_first(faces[0, r], twos[r], threes[r])

    def finish(r, ones):
        face = faces[1, r]
        second = face - step_size * (ones[1] - ones[0] - (threes[r + 1][0] - threes[r][0]))
        second_up = th_next(face, face_th[r]) - step_size * (
            ones[3] - ones[2] - (threes[r + 1][1] - threes[r][1])
        )
        second_up = jnp.where(jnp.logical_and(at_south, sub == T - 1), 0.0, second_up)
        face = faces[2, r]
        third = face - step_size * (twos[r + 1][0] - twos[r][0] - (ones[2] - ones[0]))
        third_up = ph_next(face, face_ph[r]) - step_size * (
            twos[r + 1][1] - twos[r][1] - (ones[3] - ones[1])
        )
        faces_new[1, r] = second
        faces_new[2, r] = third
        state[6, r] = 0.5 * (second + second_up)
        state[7, r] = 0.5 * (third + third_up)
        upper = firsts[r + 1]
        if r == R - 1:
            upper = jnp.where(at_top, firsts[r], upper)
        faces_new[0, r] = firsts[r]
        state[5, r] = 0.5 * (firsts[r] + upper)

    for r in range(1, R - 1):
        finish(r, edge_first(r))
    ones_low = edge_first(0)
    ones_high = edge_first(R - 1) if R > 1 else ones_low

    for t in packs + direct + [row_up, row_down, row_face]:
        t[1]()

    def outer(side, at_end, r):
        x = own(r)
        ghost = [jnp.where(at_end, x[f], from_row[side, f]) for f in range(8)]

        def column(offset, s):
            spread = jnp.broadcast_to(pack_row[s, side], (T, L))
            return jnp.sum(jnp.where(lane == sub + offset, spread, 0.0), axis=1, keepdims=True)

        right_column, left_column = column(0, 0), column(half, slots - 1)
        far = jnp.where(
            lane < half,
            jnp.broadcast_to(right_column, (T, L)),
            jnp.broadcast_to(left_column, (T, L)),
        )
        far = jnp.where(at_end, emf_second(beside(r)), far)

        def th_ghost(which, edge, at_pole, own_ghost):
            fields = [None]
            for f in range(1, 7):
                value = jnp.where(at_end, own_ghost[f], from_rowth[side, which, f - 1])
                fields.append(jnp.where(at_pole, flip(f, ghost[f][edge : edge + 1]), value))
            return emf_third(fields)

        low = th_ghost(0, 0, at_north, th_low(r))
        high = th_ghost(1, T - 1, at_south, th_high(r))
        return ghost, (emf_second(ghost), far), (emf_third(ghost), low, high)

    ghost, two, three = outer(0, at_bottom, 0)
    flux = face_flux(derived(ghost, 0), derived(own(0), 0))
    for i in range(5):
        state[i, 0] = state[i, 0] + step_size * flux[i]
    twos[0] = edge_second(two, second_parts(0))
    threes[0] = edge_third(three, third_parts(0))
    firsts[0] = advance_first(faces[0, 0], twos[0], threes[0])

    ghost, two, three = outer(1, at_top, R - 1)
    flux = face_flux(derived(own(R - 1), 0), derived(ghost, 0))
    for i in range(5):
        state[i, R - 1] = state[i, R - 1] - step_size * flux[i]
    twos[R] = edge_second(second_parts(R - 1), two)
    threes[R] = edge_third(third_parts(R - 1), three)
    firsts[R] = advance_first(face_row[...], twos[R], threes[R])

    finish(0, ones_low)
    if R > 1:
        finish(R - 1, ones_high)

    for t in transfers:
        t[2]()


def store(state, faces_new, state_hbm, faces_hbm, sem):
    copies = [
        pltpu.make_async_copy(state, state_hbm, sem.at[0]),
        pltpu.make_async_copy(faces_new, faces_hbm, sem.at[1]),
    ]
    for copy in copies:
        copy.start()
    for copy in copies:
        copy.wait()


def on_device(sizes, cells, faces):
    fields, R, T, L = cells.shape
    slots = 1 if sizes[2] == 2 else 2
    f32 = jnp.float32
    copies = 11 + slots * 5
    whole = (jax.ShapeDtypeStruct(cells.shape, f32), jax.ShapeDtypeStruct(faces.shape, f32))
    results = pl.pallas_call(
        functools.partial(kernel, sizes),
        out_shape=(pltpu.VMEM(cells.shape, f32), pltpu.VMEM(faces.shape, f32)),
        in_specs=[pl.BlockSpec(memory_space=pl.ANY)] * 2,
        out_specs=[pl.BlockSpec(memory_space=pltpu.VMEM)] * 2,
        scratch_shapes=[
            pltpu.VMEM((fields, R, T, L), f32),
            pltpu.VMEM((3, R, T, L), f32),
            pltpu.VMEM((slots, fields, R, T, L), f32),
            pltpu.VMEM((R, T, L), f32),
            pltpu.VMEM((2, 1, L), f32),
            pltpu.VMEM((slots, 2, 1, L), f32),
            pltpu.VMEM((2, fields, R, 1, L), f32),
            pltpu.VMEM((R, 1, L), f32),
            pltpu.VMEM((slots, 2, 6, R, 1, L), f32),
            pltpu.VMEM((2, fields, T, L), f32),
            pltpu.VMEM((T, L), f32),
            pltpu.VMEM((2, 2, 6, 1, L), f32),
            pltpu.SemaphoreType.DMA((2,)),
            pltpu.SemaphoreType.DMA((copies,)),
            pltpu.SemaphoreType.DMA((copies,)),
        ],
        compiler_params=pltpu.CompilerParams(collective_id=0, has_side_effects=True),
    )(cells, faces)
    return pl.pallas_call(
        store,
        out_shape=whole,
        in_specs=[pl.BlockSpec(memory_space=pltpu.VMEM)] * 2,
        out_specs=[pl.BlockSpec(memory_space=pl.ANY)] * 2,
        scratch_shapes=[pltpu.SemaphoreType.DMA((2,))],
    )(*[pltpu.with_memory_space_constraint(x, pltpu.VMEM) for x in results])


def solution(mesh):
    sizes = (mesh.shape["row"], mesh.shape["th"], mesh.shape["ph"])
    place = P(None, "row", "th", "ph")
    return jax.shard_map(
        functools.partial(on_device, sizes),
        mesh=mesh,
        in_specs=(place, place),
        out_specs=(place, place),
        check_vma=False,
    )
```
